32 devices in a mesh: data: 8 (over z, y), stage: 4 (over x, core).
Axes of the slice: x: 2, y: 2, z: 4, core: 2. Of those that a mesh axis runs over, the one named last changes fastest.
Arguments:
- master_up: float32 [4, 768, 3072], P('stage')
- master_down: float32 [4, 3072, 768], P('stage')
- mom1_up: float32 [4, 768, 3072], P('stage')
- mom1_down: float32 [4, 3072, 768], P('stage')
- mom2_up: float32 [4, 768, 3072], P('stage')
- mom2_down: float32 [4, 3072, 768], P('stage')
- grad_up: float32 [8, 4, 768, 3072], P('data', 'stage')
- grad_down: float32 [8, 4, 3072, 768], P('data', 'stage')
- stage_acts: bfloat16 [4, 16384, 768], P('stage', 'data')
- loss_grad: bfloat16 [16384, 768], P('data')
- next_batch: bfloat16 [1, 16384, 768], P(None, 'data')
- learn_rate: float32 [], replicated
- max_norm: float32 [], replicated
Outputs:
- output 1: float32 [4, 768, 3072], P('stage')
- output 2: float32 [4, 3072, 768], P('stage')
- output 3: float32 [4, 768, 3072], P('stage')
- output 4: float32 [4, 3072, 768], P('stage')
- output 5: float32 [4, 768, 3072], P('stage')
- output 6: float32 [4, 3072, 768], P('stage')
- output 7: bfloat16 [4, 1, 16384, 768], P('stage', None, 'data')
All inputs are finite; a program needn't handle non-finite values.
Results may differ from the reference program's by a relative error of at most 0.00891411.
Values are sent between devices in bfloat16 or wider.
A program may use at most 1 GiB of HBM per device.

```python
import jax
import jax.numpy as jnp
from jax import lax

STAGES = 4
REPLICAS = 8
D = 768
FF = 3072
TOKENS = 2048
MICROBATCHES = 1
ADAM_STEP = 8

ROWS = REPLICAS * TOKENS
BETA1 = 0.9
BETA2 = 0.95
ADAM_EPS = 1e-8
WEIGHT_DECAY = 0.1
NORM_EPS = 1e-6
SQRT_TWO_PI = 0.7978845608028654
GELU_CUBIC = 0.044715


def tanh_part(pre_act):
    return jnp.tanh(SQRT_TWO_PI * (pre_act + GELU_CUBIC * pre_act * pre_act * pre_act))


def gelu_tanh(pre_act):
    return 0.5 * pre_act * (1.0 + tanh_part(pre_act))


def gelu_pair(pre_act):
    tanh_val = tanh_part(pre_act)
    act_value = 0.5 * pre_act * (1.0 + tanh_val)
    act_slope = 0.5 * (1.0 + tanh_val) + 0.5 * pre_act * (1.0 - tanh_val * tanh_val) * SQRT_TWO_PI * (1.0 + 3.0 * GELU_CUBIC * pre_act * pre_act)
    return act_value, act_slope


def stage_backward(stage_in, master_up, master_down, loss_grad):
    up_bf = master_up.astype(jnp.bfloat16)
    down_bf = master_down.astype(jnp.bfloat16)

    def back_body(grad_in, stage_xs):
        rows_in, up_p, down_p = stage_xs
        pre_act = jnp.dot(rows_in, up_p, preferred_element_type=jnp.float32)
        act_value, act_slope = gelu_pair(pre_act)
        hidden = act_value.astype(jnp.bfloat16)
        d_hidden = jnp.dot(grad_in, down_p.T, preferred_element_type=jnp.float32)
        d_pre = (d_hidden * act_slope).astype(jnp.bfloat16)
        d_rows = (grad_in.astype(jnp.float32) + jnp.dot(d_pre, up_p.T, preferred_element_type=jnp.float32)).astype(jnp.bfloat16)
        dw_up = jnp.dot(rows_in.T, d_pre, preferred_element_type=jnp.float32)
        dw_down = jnp.dot(hidden.T, grad_in, preferred_element_type=jnp.float32)
        return d_rows, (dw_up, dw_down)

    _, (dw_up, dw_down) = lax.scan(back_body, loss_grad, (stage_in, up_bf, down_bf), reverse=True)
    return dw_up, dw_down


def mean_grads(grad_up, grad_down, stage_in, master_up, master_down, loss_grad):
    dw_up, dw_down = stage_backward(stage_in, master_up, master_down, loss_grad)
    gbar_up = (jnp.sum(grad_up, axis=0) + dw_up) / REPLICAS
    gbar_down = (jnp.sum(grad_down, axis=0) + dw_down) / REPLICAS
    return gbar_up, gbar_down


def adamw_update(master, first_mom, second_mom, grad_avg, clip_scale, learn_rate):
    scaled = clip_scale * grad_avg
    new_first = BETA1 * first_mom + (1.0 - BETA1) * scaled
    new_second = BETA2 * second_mom + (1.0 - BETA2) * scaled * scaled
    first_hat = new_first / (1.0 - BETA1 ** ADAM_STEP)
    second_hat = new_second / (1.0 - BETA2 ** ADAM_STEP)
    new_master = master - learn_rate * (first_hat / (jnp.sqrt(second_hat) + ADAM_EPS) + WEIGHT_DECAY * master)
    return new_master, new_first, new_second


def setup_inputs(seed: int = 0) -> dict:
    base_key = jax.random.key(seed)
    key_list = jax.random.split(base_key, 16)
    std_up = D ** -0.5
    std_down = 1.5 * (FF * STAGES) ** -0.5
    master_up = jax.random.normal(key_list[0], (STAGES, D, FF), jnp.float32) * std_up
    master_down = jax.random.normal(key_list[1], (STAGES, FF, D), jnp.float32) * std_down
    stage_acts = jax.random.normal(key_list[2], (STAGES, ROWS, D), jnp.float32).astype(jnp.bfloat16)
    loss_grad = jax.random.normal(key_list[3], (ROWS, D), jnp.float32).astype(jnp.bfloat16)
    next_batch = jax.random.normal(key_list[4], (MICROBATCHES, ROWS, D), jnp.float32).astype(jnp.bfloat16)
    grad_up = jax.random.normal(key_list[5], (REPLICAS, STAGES, D, FF), jnp.float32) * (0.4 * (TOKENS / STAGES) ** 0.5)
    grad_down = jax.random.normal(key_list[6], (REPLICAS, STAGES, FF, D), jnp.float32) * (0.6 * TOKENS ** 0.5)
    gbar_up, gbar_down = mean_grads(grad_up, grad_down, stage_acts, master_up, master_down, loss_grad)
    grad_norm = jnp.sqrt(jnp.sum(gbar_up * gbar_up) + jnp.sum(gbar_down * gbar_down))
    norm_frac = jax.random.uniform(key_list[7], (), jnp.float32, 0.35, 0.65)
    max_norm = norm_frac * grad_norm
    rms_up = norm_frac * jnp.sqrt(jnp.mean(gbar_up * gbar_up))
    rms_down = norm_frac * jnp.sqrt(jnp.mean(gbar_down * gbar_down))
    mom1_up = jax.random.normal(key_list[8], (STAGES, D, FF), jnp.float32) * (0.1 * rms_up)
    mom1_down = jax.random.normal(key_list[9], (STAGES, FF, D), jnp.float32) * (0.1 * rms_down)
    mom2_up = jax.random.uniform(key_list[10], (STAGES, D, FF), jnp.float32, 0.05, 0.15) * (rms_up * rms_up)
    mom2_down = jax.random.uniform(key_list[11], (STAGES, FF, D), jnp.float32, 0.05, 0.15) * (rms_down * rms_down)
    learn_rate = jax.random.uniform(key_list[12], (), jnp.float32, 0.1, 0.3) * std_down
    return dict(master_up=master_up, master_down=master_down, mom1_up=mom1_up, mom1_down=mom1_down, mom2_up=mom2_up, mom2_down=mom2_down, grad_up=grad_up, grad_down=grad_down, stage_acts=stage_acts, loss_grad=loss_grad, next_batch=next_batch, learn_rate=learn_rate, max_norm=max_norm)


def reference(master_up, master_down, mom1_up, mom1_down, mom2_up, mom2_down, grad_up, grad_down, stage_acts, loss_grad, next_batch, learn_rate, max_norm):
    gbar_up, gbar_down = mean_grads(grad_up, grad_down, stage_acts, master_up, master_down, loss_grad)
    grad_norm = jnp.sqrt(jnp.sum(gbar_up * gbar_up) + jnp.sum(gbar_down * gbar_down))
    clip_scale = jnp.minimum(1.0, max_norm / (grad_norm + NORM_EPS))
    new_up, new_mom1_up, new_mom2_up = adamw_update(master_up, mom1_up, mom2_up, gbar_up, clip_scale, learn_rate)
    new_down, new_mom1_down, new_mom2_down = adamw_update(master_down, mom1_down, mom2_down, gbar_down, clip_scale, learn_rate)
    up_bf = new_up.astype(jnp.bfloat16)
    down_bf = new_down.astype(jnp.bfloat16)

    def fwd_body(rows_in, weights):
        up_p, down_p = weights
        pre_act = jnp.dot(rows_in, up_p, preferred_element_type=jnp.float32)
        hidden = gelu_tanh(pre_act).astype(jnp.bfloat16)
        rows_out = (rows_in.astype(jnp.float32) + jnp.dot(hidden, down_p, preferred_element_type=jnp.float32)).astype(jnp.bfloat16)
        return rows_out, rows_out

    flat_batch = next_batch.reshape(MICROBATCHES * ROWS, D)
    _, stage_outs = lax.scan(fwd_body, flat_batch, (up_bf, down_bf))
    stage_outputs = stage_outs.reshape(STAGES, MICROBATCHES, ROWS, D)
    return (new_up, new_down, new_mom1_up, new_mom1_down, new_mom2_up, new_mom2_down, stage_outputs)
```

```python
import functools

import jax
import jax.numpy as jnp
from jax import lax
from jax.experimental import pallas as pl
from jax.experimental.pallas import tpu as pltpu
from jax.sharding import PartitionSpec as P

BETA1 = 0.9
BETA2 = 0.95
ADAM_EPS = 1e-8
WEIGHT_DECAY = 0.1
NORM_EPS = 1e-6
ADAM_STEP = 8
SQRT_TWO_PI = 0.7978845608028654
GELU_CUBIC = 0.044715
CHUNK = 256
TILE = 512
SUM_CHUNKS = 48
SUM_SKEW = 1
MESH = pl.DeviceIdType.MESH


def tanh_part(pre_act):
    return jnp.tanh(SQRT_TWO_PI * (pre_act + GELU_CUBIC * pre_act * pre_act * pre_act))


def gelu_tanh(pre_act):
    return 0.5 * pre_act * (1.0 + tanh_part(pre_act))


def gelu_pair(pre_act):
    tanh_val = tanh_part(pre_act)
    act_value = 0.5 * pre_act * (1.0 + tanh_val)
    act_slope = 0.5 * (1.0 + tanh_val) + 0.5 * pre_act * (1.0 - tanh_val * tanh_val) * SQRT_TWO_PI * (1.0 + 3.0 * GELU_CUBIC * pre_act * pre_act)
    return act_value, act_slope


def mat_tn(left, right):
    return lax.dot_general(left, right, (((0,), (0,)), ((), ())), preferred_element_type=jnp.float32)


def mat_nt(left, right):
    return lax.dot_general(left, right, (((1,), (1,)), ((), ())), preferred_element_type=jnp.float32)


def mat_nn(left, right):
    return lax.dot_general(left, right, (((1,), (0,)), ((), ())), preferred_element_type=jnp.float32)


def adamw_update(master, first_mom, second_mom, grad_avg, clip_scale, learn_rate):
    scaled = clip_scale * grad_avg
    new_first = BETA1 * first_mom + (1.0 - BETA1) * scaled
    new_second = BETA2 * second_mom + (1.0 - BETA2) * scaled * scaled
    first_hat = new_first / (1.0 - BETA1 ** ADAM_STEP)
    second_hat = new_second / (1.0 - BETA2 ** ADAM_STEP)
    new_master = master - learn_rate * (first_hat / (jnp.sqrt(second_hat) + ADAM_EPS) + WEIGHT_DECAY * master)
    return new_master, new_first, new_second


def enter(step, rep, stage, n_stages):
    @pl.when(step == 0)
    def _():
        barrier = pltpu.get_barrier_semaphore()

        @pl.when(stage > 0)
        def _():
            pl.semaphore_signal(barrier, inc=1, device_id=(rep, stage - 1), device_id_type=MESH)

        @pl.when(stage < n_stages - 1)
        def _():
            pl.semaphore_signal(barrier, inc=1, device_id=(rep, stage + 1), device_id_type=MESH)

        inner = (stage > 0) & (stage < n_stages - 1)

        @pl.when(inner)
        def _():
            pl.semaphore_wait(barrier, 2)

        @pl.when(jnp.logical_not(inner))
        def _():
            pl.semaphore_wait(barrier, 1)


def back_kernel(n_stages, n_chunks, tile, acts_ref, up_ref, down_ref, loss_ref, hid_ref, dpre_ref, gout_ref, gin, gsend, slope, send_sem, recv_sem):
    step = pl.program_id(0)
    rep = lax.axis_index('data')
    stage = lax.axis_index('stage')
    ff = up_ref.shape[1]
    enter(step, rep, stage, n_stages)

    def copy_of(idx):
        return pltpu.make_async_remote_copy(
            src_ref=gsend.at[idx],
            dst_ref=gin.at[idx],
            send_sem=send_sem.at[idx],
            recv_sem=recv_sem.at[idx],
            device_id=(rep, jnp.maximum(stage - 1, 0)),
            device_id_type=MESH,
        )

    rows_in = acts_ref[...]
    for start in range(0, ff, tile):
        cols = slice(start, start + tile)
        act_value, act_slope = gelu_pair(mat_nn(rows_in, up_ref[:, cols]))
        hid_ref[:, cols] = act_value.astype(jnp.bfloat16)
        slope[:, cols] = act_slope

    @pl.when(stage == n_stages - 1)
    def _():
        gin[step] = loss_ref[...]

    @pl.when(stage < n_stages - 1)
    def _():
        copy_of(step).wait_recv()

    grad_in = gin[step]
    gout_ref[...] = grad_in
    total = grad_in.astype(jnp.float32)
    back = jnp.zeros_like(total)
    for start in range(0, ff, tile):
        cols = slice(start, start + tile)
        d_pre = (mat_nt(grad_in, down_ref[cols, :]) * slope[:, cols]).astype(jnp.bfloat16)
        dpre_ref[:, cols] = d_pre
        back = back + mat_nt(d_pre, up_ref[:, cols])

    @pl.when(stage > 0)
    def _():
        gsend[step] = (total + back).astype(jnp.bfloat16)
        copy_of(step).start()

    @pl.when((step == n_chunks - 1) & (stage > 0))
    def _():
        for idx in range(n_chunks):
            copy_of(idx).wait_send()


def backward(n_stages, stage_in, up_bf, down_bf, loss_grad):
    rows, width = stage_in.shape
    ff = up_bf.shape[1]
    n_chunks = rows // CHUNK
    row_spec = pl.BlockSpec((CHUNK, width), lambda i: (i, 0))
    wide_spec = pl.BlockSpec((CHUNK, ff), lambda i: (i, 0))
    return pl.pallas_call(
        functools.partial(back_kernel, n_stages, n_chunks, TILE),
        grid=(n_chunks,),
        out_shape=(
            jax.ShapeDtypeStruct((rows, ff), jnp.bfloat16),
            jax.ShapeDtypeStruct((rows, ff), jnp.bfloat16),
            jax.ShapeDtypeStruct((rows, width), jnp.bfloat16),
        ),
        in_specs=[row_spec, pl.BlockSpec((width, ff), lambda i: (0, 0)), pl.BlockSpec((ff, width), lambda i: (0, 0)), row_spec],
        out_specs=(wide_spec, wide_spec, row_spec),
        scratch_shapes=[
            pltpu.VMEM((n_chunks, CHUNK, width), jnp.bfloat16),
            pltpu.VMEM((n_chunks, CHUNK, width), jnp.bfloat16),
            pltpu.VMEM((CHUNK, ff), jnp.float32),
            pltpu.SemaphoreType.DMA((n_chunks,)),
            pltpu.SemaphoreType.DMA((n_chunks,)),
        ],
        compiler_params=pltpu.CompilerParams(collective_id=0, has_side_effects=True, dimension_semantics=('arbitrary',), vmem_limit_bytes=60 * 2**20),
        name='backward',
    )(stage_in, up_bf, down_bf, loss_grad)


def fwd_kernel(n_stages, n_chunks, tile, first_ref, up_ref, down_ref, out_ref, xin, xsend, send_sem, recv_sem):
    step = pl.program_id(0)
    rep = lax.axis_index('data')
    stage = lax.axis_index('stage')
    ff = up_ref.shape[1]
    enter(step, rep, stage, n_stages)

    def copy_of(idx):
        return pltpu.make_async_remote_copy(
            src_ref=xsend.at[idx],
            dst_ref=xin.at[idx],
            send_sem=send_sem.at[idx],
            recv_sem=recv_sem.at[idx],
            device_id=(rep, jnp.minimum(stage + 1, n_stages - 1)),
            device_id_type=MESH,
        )

    @pl.when(stage == 0)
    def _():
        xin[step] = first_ref[...]

    @pl.when(stage > 0)
    def _():
        copy_of(step).wait_recv()

    rows_in = xin[step]
    total = jnp.zeros(rows_in.shape, jnp.float32)
    for start in range(0, ff, tile):
        cols = slice(start, start + tile)
        hidden = gelu_tanh(mat_nn(rows_in, up_ref[:, cols])).astype(jnp.bfloat16)
        total = total + mat_nn(hidden, down_ref[cols, :])
    rows_out = (rows_in.astype(jnp.float32) + total).astype(jnp.bfloat16)
    out_ref[...] = rows_out

    @pl.when(stage < n_stages - 1)
    def _():
        xsend[step] = rows_out
        copy_of(step).start()

    @pl.when((step == n_chunks - 1) & (stage < n_stages - 1))
    def _():
        for idx in range(n_chunks):
            copy_of(idx).wait_send()


def forward(n_stages, first_in, up_bf, down_bf):
    rows, width = first_in.shape
    ff = up_bf.shape[1]
    n_chunks = rows // CHUNK
    row_spec = pl.BlockSpec((CHUNK, width), lambda i: (i, 0))
    return pl.pallas_call(
        functools.partial(fwd_kernel, n_stages, n_chunks, TILE),
        grid=(n_chunks,),
        out_shape=jax.ShapeDtypeStruct((rows, width), jnp.bfloat16),
        in_specs=[row_spec, pl.BlockSpec((width, ff), lambda i: (0, 0)), pl.BlockSpec((ff, width), lambda i: (0, 0))],
        out_specs=row_spec,
        scratch_shapes=[
            pltpu.VMEM((n_chunks, CHUNK, width), jnp.bfloat16),
            pltpu.VMEM((n_chunks, CHUNK, width), jnp.bfloat16),
            pltpu.SemaphoreType.DMA((n_chunks,)),
            pltpu.SemaphoreType.DMA((n_chunks,)),
        ],
        compiler_params=pltpu.CompilerParams(collective_id=1, has_side_effects=True, dimension_semantics=('arbitrary',), vmem_limit_bytes=60 * 2**20),
        name='forward',
    )(first_in, up_bf, down_bf)


def sum_kernel(n_chunks, skew, up_ref, down_ref, out_up, out_down, y_up, z_up, x_up, z_down, x_down, y_down, send_sem, recv_sem, last_sem, local_sem):
    rep = lax.axis_index('data')
    stage = lax.axis_index('stage')
    z_pos = rep // 2
    y_pos = rep % 2
    inner = (z_pos == 1) | (z_pos == 2)
    outer = jnp.logical_not(inner)
    partner = rep + 1 - 2 * y_pos
    low = z_pos < 2
    near = jnp.where(low, 1 - z_pos, 5 - z_pos) * 2 + y_pos
    across = jnp.where(inner, 3 - z_pos, z_pos) * 2 + y_pos
    own_half = jnp.where(low, 0, 1)
    up_rows = up_ref.shape[0] // (2 * n_chunks)
    down_rows = down_ref.shape[0] // (2 * n_chunks)

    barrier = pltpu.get_barrier_semaphore()
    pl.semaphore_signal(barrier, inc=1, device_id=(partner, stage), device_id_type=MESH)
    pl.semaphore_signal(barrier, inc=1, device_id=(near, stage), device_id_type=MESH)

    @pl.when(inner)
    def _():
        pl.semaphore_signal(barrier, inc=1, device_id=(across, stage), device_id_type=MESH)
        pl.semaphore_wait(barrier, 3)

    @pl.when(outer)
    def _():
        pl.semaphore_wait(barrier, 2)

    def up_at(idx, half):
        return pl.ds(pl.multiple_of(idx * (2 * up_rows) + half * up_rows, up_rows), up_rows)

    def down_at(idx, half):
        return pl.ds(pl.multiple_of(idx * (2 * down_rows) + half * down_rows, down_rows), down_rows)

    def half_at(half):
        return pl.ds(pl.multiple_of(half * down_rows, down_rows), down_rows)

    def remote(src, dst, send, recv, peer):
        return pltpu.make_async_remote_copy(src_ref=src, dst_ref=dst, send_sem=send_sem.at[send], recv_sem=recv, device_id=(peer, stage), device_id_type=MESH)

    def raw_up(idx):
        return remote(up_ref.at[up_at(idx, 1 - y_pos)], y_up.at[idx], 0, recv_sem.at[0, idx], partner)

    def raw_down(idx):
        return remote(down_ref.at[pl.ds(pl.multiple_of(idx * (2 * down_rows), 2 * down_rows), 2 * down_rows)], z_down.at[idx], 1, recv_sem.at[1, idx], near)

    def pair_up(idx):
        return remote(y_up.at[idx], z_up.at[idx], 2, recv_sem.at[2, idx], near)

    def part_down(idx):
        return remote(z_down.at[idx, half_at(1 - own_half)], x_down.at[idx], 3, recv_sem.at[3, idx], across)

    def part_up(idx):
        return remote(z_up.at[idx], x_up.at[idx], 4, recv_sem.at[4, idx], across)

    def rail_down(idx):
        return remote(x_down.at[idx], y_down.at[idx], 5, recv_sem.at[5, idx], partner)

    def done_up_near(idx):
        return remote(x_up.at[idx], out_up.at[up_at(idx, y_pos)], 6, recv_sem.at[6, idx], near)

    def done_up_pair(idx):
        return remote(x_up.at[idx], out_up.at[up_at(idx, y_pos)], 7, last_sem.at[0], partner)

    def done_down_near(idx):
        return remote(y_down.at[idx], out_down.at[down_at(idx, own_half)], 8, last_sem.at[1], near)

    def done_down_across(idx):
        return remote(y_down.at[idx], out_down.at[down_at(idx, own_half)], 9, recv_sem.at[7, idx], across)

    def pass_up(idx):
        rows = up_at(idx, y_pos)
        return remote(out_up.at[rows], out_up.at[rows], 10, last_sem.at[0], partner)

    def pass_down(idx):
        rows = down_at(idx, 1 - own_half)
        return remote(out_down.at[rows], out_down.at[rows], 11, last_sem.at[1], near)

    def keep_up(idx):
        return pltpu.make_async_copy(x_up.at[idx], out_up.at[up_at(idx, y_pos)], local_sem.at[0])

    def keep_down(idx):
        return pltpu.make_async_copy(y_down.at[idx], out_down.at[down_at(idx, own_half)], local_sem.at[1])

    def valid(idx):
        return (idx >= 0) & (idx < n_chunks)

    def tick(step, carry):
        @pl.when(valid(step))
        def _():
            raw_up(step).start()

            @pl.when(outer)
            def _():
                raw_down(step).start()

        first = step - skew

        @pl.when(valid(first))
        def _():
            raw_up(first).wait_recv()
            y_up[first] = y_up[first] + up_ref[up_at(first, y_pos), :]

            @pl.when(outer)
            def _():
                pair_up(first).start()

            @pl.when(inner)
            def _():
                raw_down(first).wait_recv()
                z_down[first] = z_down[first] + down_ref[pl.ds(pl.multiple_of(first * (2 * down_rows), 2 * down_rows), 2 * down_rows), :]
                part_down(first).start()

        second = step - 2 * skew

        @pl.when(valid(second) & inner)
        def _():
            pair_up(second).wait_recv()
            z_up[second] = z_up[second] + y_up[second]
            part_up(second).start()
            part_down(second).wait_recv()
            x_down[second] = x_down[second] + z_down[second, half_at(own_half), :]
            rail_down(second).start()

        third = step - 3 * skew

        @pl.when(valid(third) & inner)
        def _():
            part_up(third).wait_recv()
            x_up[third] = x_up[third] + z_up[third]
            done_up_near(third).start()
            done_up_pair(third).start()
            keep_up(third).start()
            rail_down(third).wait_recv()
            y_down[third] = y_down[third] + x_down[third]
            done_down_across(third).start()
            done_down_near(third).start()
            keep_down(third).start()

        fourth = step - 4 * skew

        @pl.when(valid(fourth) & outer)
        def _():
            done_up_near(fourth).wait_recv()
            pass_up(fourth).start()

        @pl.when(valid(fourth) & inner)
        def _():
            remote(y_down.at[fourth], out_down.at[down_at(fourth, 1 - own_half)], 9, recv_sem.at[7, fourth], across).wait_recv()
            pass_down(fourth).start()

        return carry

    lax.fori_loop(0, n_chunks + 4 * skew, tick, 0)

    up_half = pl.ds(0, up_ref.shape[0] // 2)
    down_half = pl.ds(0, down_ref.shape[0] // 2)

    def all_up(send, recv, peer):
        return remote(up_ref.at[up_half], out_up.at[up_half], send, recv, peer)

    def all_down(send, recv, peer):
        return remote(down_ref.at[down_half], out_down.at[down_half], send, recv, peer)

    all_up(0, last_sem.at[0], partner).wait_send()
    all_up(0, last_sem.at[0], partner).wait_recv()

    @pl.when(outer)
    def _():
        remote(down_ref, out_down, 1, last_sem.at[1], near).wait_send()
        all_up(2, last_sem.at[0], near).wait_send()
        all_up(10, last_sem.at[0], partner).wait_send()
        remote(down_ref, out_down, 1, last_sem.at[1], near).wait_recv()

    @pl.when(inner)
    def _():
        all_down(3, last_sem.at[1], across).wait_send()
        all_up(4, last_sem.at[0], across).wait_send()
        all_down(5, last_sem.at[1], partner).wait_send()
        all_up(6, last_sem.at[0], near).wait_send()
        all_up(7, last_sem.at[0], partner).wait_send()
        all_down(8, last_sem.at[1], near).wait_send()
        all_down(9, last_sem.at[1], across).wait_send()
        all_down(11, last_sem.at[1], near).wait_send()
        pltpu.make_async_copy(up_ref.at[up_half], out_up.at[up_half], local_sem.at[0]).wait()
        pltpu.make_async_copy(down_ref.at[down_half], out_down.at[down_half], local_sem.at[1]).wait()


def sum_grads(grad_up, grad_down):
    n_up = grad_up.shape[0] // (2 * SUM_CHUNKS)
    n_down = grad_down.shape[0] // (2 * SUM_CHUNKS)
    up_land = pltpu.VMEM((SUM_CHUNKS, n_up, grad_up.shape[1]), jnp.float32)
    down_land = pltpu.VMEM((SUM_CHUNKS, n_down, grad_down.shape[1]), jnp.float32)
    return pl.pallas_call(
        functools.partial(sum_kernel, SUM_CHUNKS, SUM_SKEW),
        out_shape=(jax.ShapeDtypeStruct(grad_up.shape, jnp.float32), jax.ShapeDtypeStruct(grad_down.shape, jnp.float32)),
        in_specs=[pl.BlockSpec(memory_space=pltpu.VMEM)] * 2,
        out_specs=(pl.BlockSpec(memory_space=pl.ANY), pl.BlockSpec(memory_space=pl.ANY)),
        scratch_shapes=[
            up_land,
            up_land,
            up_land,
            pltpu.VMEM((SUM_CHUNKS, 2 * n_down, grad_down.shape[1]), jnp.float32),
            down_land,
            down_land,
            pltpu.SemaphoreType.DMA((12,)),
            pltpu.SemaphoreType.DMA((8, SUM_CHUNKS)),
            pltpu.SemaphoreType.DMA((2,)),
            pltpu.SemaphoreType.DMA((2,)),
        ],
        compiler_params=pltpu.CompilerParams(collective_id=2, has_side_effects=True, vmem_limit_bytes=60 * 2**20),
        name='sum_grads',
    )(grad_up, grad_down)


def solution(mesh):
    n_stages = mesh.shape['stage']
    n_reps = mesh.shape['data']

    def local_step(master_up, master_down, mom1_up, mom1_down, mom2_up, mom2_down, grad_up, grad_down, stage_acts, loss_grad, next_batch, learn_rate, max_norm):
        stage_in = stage_acts[0]
        up_bf = master_up[0].astype(jnp.bfloat16)
        down_bf = master_down[0].astype(jnp.bfloat16)
        hid_own, dpre_own, grad_own = backward(n_stages, stage_in, up_bf, down_bf, loss_grad)

        sum_up, sum_down = sum_grads(grad_up[0, 0] + mat_tn(stage_in, dpre_own), grad_down[0, 0] + mat_tn(hid_own, grad_own))
        gbar_up = sum_up / n_reps
        gbar_down = sum_down / n_reps
        local_sq = jnp.sum(gbar_up * gbar_up) + jnp.sum(gbar_down * gbar_down)
        grad_norm = jnp.sqrt(lax.psum(local_sq, 'stage'))
        clip_scale = jnp.minimum(1.0, max_norm / (grad_norm + NORM_EPS))
        new_up, new_m1_up, new_m2_up = adamw_update(master_up[0], mom1_up[0], mom2_up[0], gbar_up, clip_scale, learn_rate)
        new_down, new_m1_down, new_m2_down = adamw_update(master_down[0], mom1_down[0], mom2_down[0], gbar_down, clip_scale, learn_rate)
        stage_out = forward(n_stages, next_batch[0], new_up.astype(jnp.bfloat16), new_down.astype(jnp.bfloat16))
        return (new_up[None], new_down[None], new_m1_up[None], new_m1_down[None], new_m2_up[None], new_m2_down[None], stage_out[None, None])

    w_spec = P('stage', None, None)
    g_spec = P('data', 'stage', None, None)
    in_specs = (w_spec, w_spec, w_spec, w_spec, w_spec, w_spec, g_spec, g_spec, P('stage', 'data', None), P('data', None), P(None, 'data', None), P(), P())
    out_specs = (w_spec, w_spec, w_spec, w_spec, w_spec, w_spec, P('stage', None, 'data', None))
    return jax.shard_map(local_step, mesh=mesh, in_specs=in_specs, out_specs=out_specs, check_vma=False)
```

```python
import functools

import jax
import jax.numpy as jnp
from jax import lax
from jax.experimental import pallas as pl
from jax.experimental.pallas import tpu as pltpu
from jax.sharding import PartitionSpec as P

BETA1 = 0.9
BETA2 = 0.95
ADAM_EPS = 1e-8
WEIGHT_DECAY = 0.1
NORM_EPS = 1e-6
ADAM_STEP = 8
SQRT_TWO_PI = 0.7978845608028654
GELU_CUBIC = 0.044715
CHUNK = 256
TILE = 768
LANES = 128
ADAM_BLOCKS = 6
SUM_SKEW = 1
MESH = pl.DeviceIdType.MESH


def tanh_part(pre_act):
    return jnp.tanh(SQRT_TWO_PI * (pre_act + GELU_CUBIC * pre_act * pre_act * pre_act))


def gelu_tanh(pre_act):
    return 0.5 * pre_act * (1.0 + tanh_part(pre_act))


def gelu_pair(pre_act):
    tanh_val = tanh_part(pre_act)
    act_value = 0.5 * pre_act * (1.0 + tanh_val)
    act_slope = 0.5 * (1.0 + tanh_val) + 0.5 * pre_act * (1.0 - tanh_val * tanh_val) * SQRT_TWO_PI * (1.0 + 3.0 * GELU_CUBIC * pre_act * pre_act)
    return act_value, act_slope


def mat_tn(left, right):
    return lax.dot_general(left, right, (((0,), (0,)), ((), ())), preferred_element_type=jnp.float32)


def mat_nt(left, right):
    return lax.dot_general(left, right, (((1,), (1,)), ((), ())), preferred_element_type=jnp.float32)


def mat_nn(left, right):
    return lax.dot_general(left, right, (((1,), (0,)), ((), ())), preferred_element_type=jnp.float32)


def adamw_update(master, first_mom, second_mom, grad_avg, clip_scale, learn_rate):
    scaled = clip_scale * grad_avg
    new_first = BETA1 * first_mom + (1.0 - BETA1) * scaled
    new_second = BETA2 * second_mom + (1.0 - BETA2) * scaled * scaled
    first_hat = new_first * (1.0 / (1.0 - BETA1 ** ADAM_STEP))
    second_hat = new_second * (1.0 / (1.0 - BETA2 ** ADAM_STEP))
    new_master = master - learn_rate * (first_hat / (jnp.sqrt(second_hat) + ADAM_EPS) + WEIGHT_DECAY * master)
    return new_master, new_first, new_second


def enter(step, rep, stage, n_stages):
    @pl.when(step == 0)
    def _():
        barrier = pltpu.get_barrier_semaphore()

        @pl.when(stage > 0)
        def _():
            pl.semaphore_signal(barrier, inc=1, device_id=(rep, stage - 1), device_id_type=MESH)

        @pl.when(stage < n_stages - 1)
        def _():
            pl.semaphore_signal(barrier, inc=1, device_id=(rep, stage + 1), device_id_type=MESH)

        inner = (stage > 0) & (stage < n_stages - 1)

        @pl.when(inner)
        def _():
            pl.semaphore_wait(barrier, 2)

        @pl.when(jnp.logical_not(inner))
        def _():
            pl.semaphore_wait(barrier, 1)


def put_blocks(ref, start, value):
    for offset in range(0, value.shape[1], LANES):
        ref[(start + offset) // LANES] = value[:, offset : offset + LANES]


def round_rows(src_ref, dst_ref, rows):
    def body(idx, carry):
        block = pl.ds(pl.multiple_of(idx * rows, rows), rows)
        dst_ref[block, :] = src_ref[block, :].astype(jnp.bfloat16)
        return carry

    lax.fori_loop(0, src_ref.shape[0] // rows, body, 0)


def back_kernel(n_stages, n_chunks, tile, acts_ref, up_hbm, down_hbm, loss_ref, hid_ref, dpre_ref, gout_ref, flip_ref, up_ref, down_ref, gin, gsend, slope, send_sem, recv_sem):
    step = pl.program_id(0)
    rep = lax.axis_index('data')
    stage = lax.axis_index('stage')
    ff = up_ref.shape[1]
    enter(step, rep, stage, n_stages)

    def copy_of(idx):
        return pltpu.make_async_remote_copy(
            src_ref=gsend.at[idx],
            dst_ref=gin.at[idx],
            send_sem=send_sem.at[idx],
            recv_sem=recv_sem.at[idx],
            device_id=(rep, jnp.maximum(stage - 1, 0)),
            device_id_type=MESH,
        )

    def ahead(rows_in, cols):
        act_value, act_slope = gelu_pair(mat_nn(rows_in, up_ref[:, cols]))
        put_blocks(hid_ref, cols.start, act_value.astype(jnp.bfloat16))
        slope[:, cols] = act_slope

    @pl.when(step == 0)
    def _():
        round_rows(up_hbm, up_ref, 64)
        round_rows(down_hbm, down_ref, 256)
        rows_in = acts_ref[...]
        flip_ref[...] = rows_in.T
        for start in range(0, ff, tile):
            ahead(rows_in, slice(start, start + tile))

    @pl.when(step > 0)
    def _():
        idx = step - 1

        @pl.when(stage == n_stages - 1)
        def _():
            gin[idx] = loss_ref[...]

        @pl.when(stage < n_stages - 1)
        def _():
            copy_of(idx).wait_recv()

        grad_in = gin[idx]
        gout_ref[...] = grad_in
        rows_in = acts_ref[...]
        flip_ref[...] = rows_in.T
        back = jnp.zeros(grad_in.shape, jnp.float32)
        for start in range(0, ff, tile):
            cols = slice(start, start + tile)
            d_pre = (mat_nt(grad_in, down_ref[cols, :]) * slope[:, cols]).astype(jnp.bfloat16)
            put_blocks(dpre_ref, start, d_pre)
            back = back + mat_nt(d_pre, up_ref[:, cols])
            ahead(rows_in, cols)

        @pl.when(stage > 0)
        def _():
            gsend[idx] = (grad_in.astype(jnp.float32) + back).astype(jnp.bfloat16)
            copy_of(idx).start()

    @pl.when((step == n_chunks) & (stage > 0))
    def _():
        for idx in range(n_chunks):
            copy_of(idx).wait_send()


def backward(n_stages, stage_in, master_up, master_down, loss_grad):
    rows, width = stage_in.shape
    ff = master_up.shape[1]
    n_chunks = rows // CHUNK

    def now(i):
        return jnp.minimum(i, n_chunks - 1)

    def late(i):
        return jnp.maximum(i - 1, 0)

    return pl.pallas_call(
        functools.partial(back_kernel, n_stages, n_chunks, TILE),
        grid=(n_chunks + 1,),
        out_shape=(
            jax.ShapeDtypeStruct((ff // LANES, rows, LANES), jnp.bfloat16),
            jax.ShapeDtypeStruct((ff // LANES, rows, LANES), jnp.bfloat16),
            jax.ShapeDtypeStruct((rows, width), jnp.bfloat16),
            jax.ShapeDtypeStruct((width, rows), jnp.bfloat16),
        ),
        in_specs=[
            pl.BlockSpec((CHUNK, width), lambda i: (now(i), 0)),
            pl.BlockSpec(memory_space=pltpu.VMEM),
            pl.BlockSpec(memory_space=pltpu.VMEM),
            pl.BlockSpec((CHUNK, width), lambda i: (late(i), 0)),
        ],
        out_specs=(
            pl.BlockSpec((ff // LANES, CHUNK, LANES), lambda i: (0, now(i), 0)),
            pl.BlockSpec((ff // LANES, CHUNK, LANES), lambda i: (0, late(i), 0)),
            pl.BlockSpec((CHUNK, width), lambda i: (late(i), 0)),
            pl.BlockSpec((width, CHUNK), lambda i: (0, now(i))),
        ),
        scratch_shapes=[
            pltpu.VMEM((width, ff), jnp.bfloat16),
            pltpu.VMEM((ff, width), jnp.bfloat16),
            pltpu.VMEM((n_chunks, CHUNK, width), jnp.bfloat16),
            pltpu.VMEM((n_chunks, CHUNK, width), jnp.bfloat16),
            pltpu.VMEM((CHUNK, ff), jnp.float32),
            pltpu.SemaphoreType.DMA((n_chunks,)),
            pltpu.SemaphoreType.DMA((n_chunks,)),
        ],
        compiler_params=pltpu.CompilerParams(collective_id=0, has_side_effects=True, dimension_semantics=('arbitrary',), vmem_limit_bytes=67043328),
        name='backward',
    )(stage_in, master_up, master_down, loss_grad)


def fwd_kernel(n_stages, n_chunks, tile, first_ref, up_ref, down_ref, out_ref, xin, xsend, send_sem, recv_sem):
    step = pl.program_id(0)
    rep = lax.axis_index('data')
    stage = lax.axis_index('stage')
    ff = up_ref.shape[1]
    enter(step, rep, stage, n_stages)

    def copy_of(idx):
        return pltpu.make_async_remote_copy(
            src_ref=xsend.at[idx],
            dst_ref=xin.at[idx],
            send_sem=send_sem.at[idx],
            recv_sem=recv_sem.at[idx],
            device_id=(rep, jnp.minimum(stage + 1, n_stages - 1)),
            device_id_type=MESH,
        )

    @pl.when(stage == 0)
    def _():
        xin[step] = first_ref[...]

    @pl.when(stage > 0)
    def _():
        copy_of(step).wait_recv()

    rows_in = xin[step]
    total = jnp.zeros(rows_in.shape, jnp.float32)
    for start in range(0, ff, tile):
        cols = slice(start, start + tile)
        hidden = gelu_tanh(mat_nn(rows_in, up_ref[:, cols])).astype(jnp.bfloat16)
        total = total + mat_nn(hidden, down_ref[cols, :])
    rows_out = (rows_in.astype(jnp.float32) + total).astype(jnp.bfloat16)
    out_ref[...] = rows_out

    @pl.when(stage < n_stages - 1)
    def _():
        xsend[step] = rows_out
        copy_of(step).start()

    @pl.when((step == n_chunks - 1) & (stage < n_stages - 1))
    def _():
        for idx in range(n_chunks):
            copy_of(idx).wait_send()


def forward(n_stages, first_in, up_bf, down_bf):
    rows, width = first_in.shape
    ff = up_bf.shape[1]
    n_chunks = rows // CHUNK
    row_spec = pl.BlockSpec((CHUNK, width), lambda i: (i, 0))
    return pl.pallas_call(
        functools.partial(fwd_kernel, n_stages, n_chunks, TILE),
        grid=(n_chunks,),
        out_shape=jax.ShapeDtypeStruct((rows, width), jnp.bfloat16),
        in_specs=[row_spec, pl.BlockSpec((width, ff), lambda i: (0, 0)), pl.BlockSpec((ff, width), lambda i: (0, 0))],
        out_specs=row_spec,
        scratch_shapes=[
            pltpu.VMEM((n_chunks, CHUNK, width), jnp.bfloat16),
            pltpu.VMEM((n_chunks, CHUNK, width), jnp.bfloat16),
            pltpu.SemaphoreType.DMA((n_chunks,)),
            pltpu.SemaphoreType.DMA((n_chunks,)),
        ],
        compiler_params=pltpu.CompilerParams(collective_id=1, has_side_effects=True, dimension_semantics=('arbitrary',), vmem_limit_bytes=60 * 2**20),
        name='forward',
    )(first_in, up_bf, down_bf)


def fold_squares(value):
    total = jnp.zeros((8, LANES), jnp.float32)
    for row in range(0, value.shape[0], 8):
        for col in range(0, value.shape[1], LANES):
            part = value[row : row + 8, col : col + LANES]
            total = total + part * part
    return total


def sum_kernel(n_chunks, skew, n_reps, flip_ref, dpre_hbm, hid_hbm, gown_ref, gup_hbm, gdown_hbm, out_up, out_down, sq_ref, acc_up, acc_down, dpre_buf, hid_buf, y_up, z_up, x_up, z_down, x_down, y_down, send_sem, recv_sem, last_sem, local_sem, load_sem, grad_sem, sq_part, sq_land, sq_send, sq_recv):
    rep = lax.axis_index('data')
    stage = lax.axis_index('stage')
    z_pos = rep // 2
    y_pos = rep % 2
    inner = (z_pos == 1) | (z_pos == 2)
    outer = jnp.logical_not(inner)
    partner = rep + 1 - 2 * y_pos
    low = z_pos < 2
    near = jnp.where(low, 1 - z_pos, 5 - z_pos) * 2 + y_pos
    across = jnp.where(inner, 3 - z_pos, z_pos) * 2 + y_pos
    own_half = jnp.where(low, 0, 1)
    n_blocks = n_chunks // 2
    up_rows = out_up.shape[0] // 4
    down_rows = out_down.shape[0] // (2 * n_chunks)

    def load_dpre(block):
        slot = lax.rem(block, 2)
        return pltpu.make_async_copy(dpre_hbm.at[block], dpre_buf.at[slot], load_sem.at[0, slot])

    def load_hid(block):
        slot = lax.rem(block, 2)
        return pltpu.make_async_copy(hid_hbm.at[block], hid_buf.at[slot], load_sem.at[1, slot])

    def load_gup(block):
        return pltpu.make_async_copy(gup_hbm.at[:, pl.ds(pl.multiple_of(block * LANES, LANES), LANES)], acc_up.at[block], grad_sem.at[0, block])

    def load_gdown(block):
        return pltpu.make_async_copy(gdown_hbm.at[pl.ds(pl.multiple_of(block * LANES, LANES), LANES)], acc_down.at[block], grad_sem.at[1, block])

    def build(block):
        slot = lax.rem(block, 2)
        load_dpre(block).wait()
        load_gup(block).wait()
        acc_up[block] = acc_up[block] + mat_nn(flip_ref[...], dpre_buf[slot])
        load_hid(block).wait()
        load_gdown(block).wait()
        acc_down[block] = acc_down[block] + mat_tn(hid_buf[slot], gown_ref[...])

        @pl.when(block + 2 < n_blocks)
        def _():
            load_dpre(block + 2).start()
            load_hid(block + 2).start()

    for block in range(2):
        load_dpre(block).start()
        load_gup(block).start()
        load_hid(block).start()
        load_gdown(block).start()

    def load_rest(block, carry):
        load_gup(block).start()
        load_gdown(block).start()
        return carry

    lax.fori_loop(2, n_blocks, load_rest, 0)
    sq_part[...] = jnp.zeros_like(sq_part)
    build(0)

    barrier = pltpu.get_barrier_semaphore()
    for hop in range(1, n_reps):
        pl.semaphore_signal(barrier, inc=1, device_id=(lax.rem(rep + hop, n_reps), stage), device_id_type=MESH)
    pl.semaphore_wait(barrier, n_reps - 1)

    def rows_at(idx, half):
        return pl.ds(pl.multiple_of((half * 2 + lax.rem(idx, 2)) * up_rows, up_rows), up_rows)

    def up_out(idx, half):
        return out_up.at[rows_at(idx, half), pl.ds(pl.multiple_of((idx // 2) * LANES, LANES), LANES)]

    def pair_at(idx):
        return pl.ds(pl.multiple_of(lax.rem(idx, 2) * (2 * down_rows), 2 * down_rows), 2 * down_rows)

    def down_at(idx, half):
        return pl.ds(pl.multiple_of(idx * (2 * down_rows) + half * down_rows, down_rows), down_rows)

    def half_at(half):
        return pl.ds(pl.multiple_of(half * down_rows, down_rows), down_rows)

    def remote(src, dst, send, recv, peer):
        return pltpu.make_async_remote_copy(src_ref=src, dst_ref=dst, send_sem=send_sem.at[send], recv_sem=recv, device_id=(peer, stage), device_id_type=MESH)

    def raw_up(idx):
        return remote(acc_up.at[idx // 2, rows_at(idx, 1 - y_pos)], y_up.at[idx], 0, recv_sem.at[0, idx], partner)

    def raw_down(idx):
        return remote(acc_down.at[idx // 2, pair_at(idx)], z_down.at[idx], 1, recv_sem.at[1, idx], near)

    def pair_up(idx):
        return remote(y_up.at[idx], z_up.at[idx], 2, recv_sem.at[2, idx], near)

    def part_down(idx):
        return remote(z_down.at[idx, half_at(1 - own_half)], x_down.at[idx], 3, recv_sem.at[3, idx], across)

    def part_up(idx):
        return remote(z_up.at[idx], x_up.at[idx], 4, recv_sem.at[4, idx], across)

    def rail_down(idx):
        return remote(x_down.at[idx], y_down.at[idx], 5, recv_sem.at[5, idx], partner)

    def done_up_near(idx):
        return remote(x_up.at[idx], up_out(idx, y_pos), 6, recv_sem.at[6, idx], near)

    def done_up_pair(idx):
        return remote(x_up.at[idx], up_out(idx, y_pos), 7, last_sem.at[0], partner)

    def done_down_near(idx):
        return remote(y_down.at[idx], out_down.at[down_at(idx, own_half)], 8, last_sem.at[1], near)

    def done_down_across(idx):
        return remote(y_down.at[idx], out_down.at[down_at(idx, own_half)], 9, recv_sem.at[7, idx], across)

    def pass_up(idx):
        return remote(up_out(idx, y_pos), up_out(idx, y_pos), 10, last_sem.at[0], partner)

    def pass_down(idx):
        rows = down_at(idx, 1 - own_half)
        return remote(out_down.at[rows], out_down.at[rows], 11, last_sem.at[1], near)

    def keep_up(idx):
        return pltpu.make_async_copy(x_up.at[idx], up_out(idx, y_pos), local_sem.at[0])

    def keep_down(idx):
        return pltpu.make_async_copy(y_down.at[idx], out_down.at[down_at(idx, own_half)], local_sem.at[1])

    def valid(idx):
        return (idx >= 0) & (idx < n_chunks)

    def tick(step, carry):
        @pl.when(valid(step))
        def _():
            raw_up(step).start()

            @pl.when(outer)
            def _():
                raw_down(step).start()

        first = step - skew

        @pl.when(valid(first))
        def _():
            raw_up(first).wait_recv()
            y_up[first] = y_up[first] + acc_up[first // 2, rows_at(first, y_pos), :]

            @pl.when(outer)
            def _():
                pair_up(first).start()

            @pl.when(inner)
            def _():
                raw_down(first).wait_recv()
                z_down[first] = z_down[first] + acc_down[first // 2, pair_at(first), :]
                part_down(first).start()

        second = step - 2 * skew

        @pl.when(valid(second) & inner)
        def _():
            pair_up(second).wait_recv()
            z_up[second] = z_up[second] + y_up[second]
            part_up(second).start()
            part_down(second).wait_recv()
            x_down[second] = x_down[second] + z_down[second, half_at(own_half), :]
            rail_down(second).start()

        third = step - 3 * skew

        @pl.when(valid(third) & inner)
        def _():
            part_up(third).wait_recv()
            total_up = x_up[third] + z_up[third]
            x_up[third] = total_up
            sq_part[0] = sq_part[0] + fold_squares(total_up / n_reps)
            done_up_near(third).start()
            done_up_pair(third).start()
            keep_up(third).start()
            rail_down(third).wait_recv()
            total_down = y_down[third] + x_down[third]
            y_down[third] = total_down
            sq_part[1] = sq_part[1] + fold_squares(total_down / n_reps)
            done_down_across(third).start()
            done_down_near(third).start()
            keep_down(third).start()

        fourth = step - 4 * skew

        @pl.when(valid(fourth) & outer)
        def _():
            done_up_near(fourth).wait_recv()
            pass_up(fourth).start()

        @pl.when(valid(fourth) & inner)
        def _():
            remote(y_down.at[fourth], out_down.at[down_at(fourth, 1 - own_half)], 9, recv_sem.at[7, fourth], across).wait_recv()
            pass_down(fourth).start()

        @pl.when((lax.rem(step, 2) == 1) & (step + 1 < n_chunks))
        def _():
            build((step + 1) // 2)

        return carry

    lax.fori_loop(0, n_chunks + 4 * skew, tick, 0)

    slot = jnp.where(low, 0, 2) + y_pos

    def square_copy(hop, source):
        return pltpu.make_async_remote_copy(src_ref=sq_land.at[source], dst_ref=sq_land.at[source], send_sem=sq_send.at[hop - 1], recv_sem=sq_recv.at[source], device_id=(lax.rem(rep + hop, n_reps), stage), device_id_type=MESH)

    @pl.when(inner)
    def _():
        sq_land[slot] = jnp.where(z_pos == 1, sq_part[0], 0.0) + jnp.where(y_pos == 0, sq_part[1], 0.0)
        for hop in range(1, n_reps):
            square_copy(hop, slot).start()

    up_half = pl.ds(0, out_up.shape[0] // 2)
    down_half = pl.ds(0, out_down.shape[0] // 2)

    def all_up(send, recv, peer):
        return remote(out_up.at[up_half], out_up.at[up_half], send, recv, peer)

    def all_down(send, recv, peer):
        return remote(out_down.at[down_half], out_down.at[down_half], send, recv, peer)

    all_up(0, last_sem.at[0], partner).wait_send()
    all_up(0, last_sem.at[0], partner).wait_recv()

    @pl.when(outer)
    def _():
        remote(out_down, out_down, 1, last_sem.at[1], near).wait_send()
        all_up(2, last_sem.at[0], near).wait_send()
        all_up(10, last_sem.at[0], partner).wait_send()
        remote(out_down, out_down, 1, last_sem.at[1], near).wait_recv()

    @pl.when(inner)
    def _():
        all_down(3, last_sem.at[1], across).wait_send()
        all_up(4, last_sem.at[0], across).wait_send()
        all_down(5, last_sem.at[1], partner).wait_send()
        all_up(6, last_sem.at[0], near).wait_send()
        all_up(7, last_sem.at[0], partner).wait_send()
        all_down(8, last_sem.at[1], near).wait_send()
        all_down(9, last_sem.at[1], across).wait_send()
        all_down(11, last_sem.at[1], near).wait_send()
        pltpu.make_async_copy(out_up.at[up_half], out_up.at[up_half], local_sem.at[0]).wait()
        pltpu.make_async_copy(out_down.at[down_half], out_down.at[down_half], local_sem.at[1]).wait()

    for source in range(4):
        @pl.when(rep != source + 2)
        def _():
            square_copy(1, source).wait_recv()

    @pl.when(inner)
    def _():
        for hop in range(1, n_reps):
            square_copy(hop, slot).wait_send()

    sq_ref[...] = sq_land[0] + sq_land[1] + sq_land[2] + sq_land[3]


def sum_grads(n_reps, flipped, dpre_own, hid_own, grad_own, grad_up, grad_down):
    width, ff = grad_up.shape
    rows = grad_own.shape[0]
    n_blocks = ff // LANES
    n_chunks = 2 * n_blocks
    up_land = pltpu.VMEM((n_chunks, width // 4, LANES), jnp.float32)
    down_land = pltpu.VMEM((n_chunks, LANES // 4, width), jnp.float32)
    vmem = pl.BlockSpec(memory_space=pltpu.VMEM)
    hbm = pl.BlockSpec(memory_space=pl.ANY)
    return pl.pallas_call(
        functools.partial(sum_kernel, n_chunks, SUM_SKEW, n_reps),
        out_shape=(jax.ShapeDtypeStruct(grad_up.shape, jnp.float32), jax.ShapeDtypeStruct(grad_down.shape, jnp.float32), jax.ShapeDtypeStruct((8, LANES), jnp.float32)),
        in_specs=[vmem, hbm, hbm, vmem, hbm, hbm],
        out_specs=(hbm, hbm, vmem),
        scratch_shapes=[
            pltpu.VMEM((n_blocks, width, LANES), jnp.float32),
            pltpu.VMEM((n_blocks, LANES, width), jnp.float32),
            pltpu.VMEM((2, rows, LANES), jnp.bfloat16),
            pltpu.VMEM((2, rows, LANES), jnp.bfloat16),
            up_land,
            up_land,
            up_land,
            pltpu.VMEM((n_chunks, LANES // 2, width), jnp.float32),
            down_land,
            down_land,
            pltpu.SemaphoreType.DMA((12,)),
            pltpu.SemaphoreType.DMA((8, n_chunks)),
            pltpu.SemaphoreType.DMA((2,)),
            pltpu.SemaphoreType.DMA((2,)),
            pltpu.SemaphoreType.DMA((2, 2)),
            pltpu.SemaphoreType.DMA((2, n_blocks)),
            pltpu.VMEM((2, 8, LANES), jnp.float32),
            pltpu.VMEM((4, 8, LANES), jnp.float32),
            pltpu.SemaphoreType.DMA((n_reps - 1,)),
            pltpu.SemaphoreType.DMA((4,)),
        ],
        compiler_params=pltpu.CompilerParams(collective_id=2, has_side_effects=True, vmem_limit_bytes=67043328),
        name='sum_grads',
    )(flipped, dpre_own, hid_own, grad_own, grad_up, grad_down)


def adam_kernel(n_reps, scale_ref, master_ref, first_ref, second_ref, sum_ref, new_master, new_first, new_second, new_bf):
    result, first_mom, second_mom = adamw_update(master_ref[...], first_ref[...], second_ref[...], sum_ref[...] / n_reps, scale_ref[0], scale_ref[1])
    new_master[...] = result
    new_first[...] = first_mom
    new_second[...] = second_mom
    new_bf[...] = result.astype(jnp.bfloat16)


def adam(n_reps, scales, master, first_mom, second_mom, grad_sum):
    rows, cols = master.shape
    block = pl.BlockSpec((rows // ADAM_BLOCKS, cols), lambda i: (i, 0))
    full = jax.ShapeDtypeStruct(master.shape, jnp.float32)
    return pl.pallas_call(
        functools.partial(adam_kernel, n_reps),
        grid=(ADAM_BLOCKS,),
        out_shape=(full, full, full, jax.ShapeDtypeStruct(master.shape, jnp.bfloat16)),
        in_specs=[pl.BlockSpec(memory_space=pltpu.SMEM), block, block, block, block],
        out_specs=(block, block, block, block),
        compiler_params=pltpu.CompilerParams(dimension_semantics=('arbitrary',), vmem_limit_bytes=60 * 2**20),
        name='adam',
    )(scales, master, first_mom, second_mom, grad_sum)


def solution(mesh):
    n_stages = mesh.shape['stage']
    n_reps = mesh.shape['data']

    def local_step(master_up, master_down, mom1_up, mom1_down, mom2_up, mom2_down, grad_up, grad_down, stage_acts, loss_grad, next_batch, learn_rate, max_norm):
        stage_in = stage_acts[0]
        hid_own, dpre_own, grad_own, flipped = backward(n_stages, stage_in, master_up[0], master_down[0], loss_grad)
        sum_up, sum_down, squares = sum_grads(n_reps, flipped, dpre_own, hid_own, grad_own, grad_up[0, 0], grad_down[0, 0])
        grad_norm = jnp.sqrt(lax.psum(jnp.sum(squares), 'stage'))
        clip_scale = jnp.minimum(1.0, max_norm / (grad_norm + NORM_EPS))
        scales = jnp.stack([clip_scale, learn_rate])
        new_up, new_m1_up, new_m2_up, up_bf = adam(n_reps, scales, master_up[0], mom1_up[0], mom2_up[0], sum_up)
        new_down, new_m1_down, new_m2_down, down_bf = adam(n_reps, scales, master_down[0], mom1_down[0], mom2_down[0], sum_down)
        stage_out = forward(n_stages, next_batch[0], up_bf, down_bf)
        return (new_up[None], new_down[None], new_m1_up[None], new_m1_down[None], new_m2_up[None], new_m2_down[None], stage_out[None, None])

    w_spec = P('stage', None, None)
    g_spec = P('data', 'stage', None, None)
    in_specs = (w_spec, w_spec, w_spec, w_spec, w_spec, w_spec, g_spec, g_spec, P('stage', 'data', None), P('data', None), P(None, 'data', None), P(), P())
    out_specs = (w_spec, w_spec, w_spec, w_spec, w_spec, w_spec, P('stage', None, 'data', None))
    return jax.shard_map(local_step, mesh=mesh, in_specs=in_specs, out_specs=out_specs, check_vma=False)
```

```python
import functools

import jax
import jax.numpy as jnp
from jax import lax
from jax.experimental import pallas as pl
from jax.experimental.pallas import tpu as pltpu
from jax.sharding import PartitionSpec as P

BETA1 = 0.9
BETA2 = 0.95
ADAM_EPS = 1e-8
WEIGHT_DECAY = 0.1
NORM_EPS = 1e-6
ADAM_STEP = 8
SQRT_TWO_PI = 0.7978845608028654
GELU_CUBIC = 0.044715
CHUNK = 256
TILE = 768
LANES = 128
ADAM_BLOCKS = 8
FWD_CHUNK = 128
FWD_TILE = 1536
SUM_SKEW = 1
MESH = pl.DeviceIdType.MESH


def tanh_part(pre_act):
    return jnp.tanh(SQRT_TWO_PI * (pre_act + GELU_CUBIC * pre_act * pre_act * pre_act))


def gelu_tanh(pre_act):
    return 0.5 * pre_act * (1.0 + tanh_part(pre_act))


def gelu_pair(pre_act):
    tanh_val = tanh_part(pre_act)
    act_value = 0.5 * pre_act * (1.0 + tanh_val)
    act_slope = 0.5 * (1.0 + tanh_val) + 0.5 * pre_act * (1.0 - tanh_val * tanh_val) * SQRT_TWO_PI * (1.0 + 3.0 * GELU_CUBIC * pre_act * pre_act)
    return act_value, act_slope


def mat_tn(left, right):
    return lax.dot_general(left, right, (((0,), (0,)), ((), ())), preferred_element_type=jnp.float32)


def mat_nt(left, right):
    return lax.dot_general(left, right, (((1,), (1,)), ((), ())), preferred_element_type=jnp.float32)


def mat_nn(left, right):
    return lax.dot_general(left, right, (((1,), (0,)), ((), ())), preferred_element_type=jnp.float32)


def adamw_update(master, first_mom, second_mom, grad_avg, clip_scale, learn_rate):
    scaled = clip_scale * grad_avg
    new_first = BETA1 * first_mom + (1.0 - BETA1) * scaled
    new_second = BETA2 * second_mom + (1.0 - BETA2) * scaled * scaled
    first_hat = new_first * (1.0 / (1.0 - BETA1 ** ADAM_STEP))
    second_hat = new_second * (1.0 / (1.0 - BETA2 ** ADAM_STEP))
    new_master = master - learn_rate * (first_hat / (jnp.sqrt(second_hat) + ADAM_EPS) + WEIGHT_DECAY * master)
    return new_master, new_first, new_second


def enter(step, rep, stage, n_stages):
    @pl.when(step == 0)
    def _():
        barrier = pltpu.get_barrier_semaphore()

        @pl.when(stage > 0)
        def _():
            pl.semaphore_signal(barrier, inc=1, device_id=(rep, stage - 1), device_id_type=MESH)

        @pl.when(stage < n_stages - 1)
        def _():
            pl.semaphore_signal(barrier, inc=1, device_id=(rep, stage + 1), device_id_type=MESH)

        inner = (stage > 0) & (stage < n_stages - 1)

        @pl.when(inner)
        def _():
            pl.semaphore_wait(barrier, 2)

        @pl.when(jnp.logical_not(inner))
        def _():
            pl.semaphore_wait(barrier, 1)


def put_blocks(ref, start, value):
    for offset in range(0, value.shape[1], LANES):
        ref[(start + offset) // LANES] = value[:, offset : offset + LANES]


def round_rows(src_ref, dst_ref, rows):
    def body(idx, carry):
        block = pl.ds(pl.multiple_of(idx * rows, rows), rows)
        dst_ref[block, :] = src_ref[block, :].astype(jnp.bfloat16)
        return carry

    lax.fori_loop(0, src_ref.shape[0] // rows, body, 0)


def back_kernel(n_stages, n_chunks, tile, acts_ref, up_hbm, down_hbm, loss_ref, hid_ref, dpre_ref, gout_ref, flip_ref, up_ref, down_ref, gin, gsend, slope, send_sem, recv_sem):
    step = pl.program_id(0)
    rep = lax.axis_index('data')
    stage = lax.axis_index('stage')
    ff = up_ref.shape[1]
    enter(step, rep, stage, n_stages)

    def copy_of(idx):
        return pltpu.make_async_remote_copy(
            src_ref=gsend.at[idx],
            dst_ref=gin.at[idx],
            send_sem=send_sem.at[idx],
            recv_sem=recv_sem.at[idx],
            device_id=(rep, jnp.maximum(stage - 1, 0)),
            device_id_type=MESH,
        )

    def ahead(rows_in, cols):
        act_value, act_slope = gelu_pair(mat_nn(rows_in, up_ref[:, cols]))
        put_blocks(hid_ref, cols.start, act_value.astype(jnp.bfloat16))
        slope[:, cols] = act_slope

    @pl.when(step == 0)
    def _():
        round_rows(up_hbm, up_ref, 64)
        round_rows(down_hbm, down_ref, 256)
        rows_in = acts_ref[...]
        flip_ref[...] = rows_in.T
        for start in range(0, ff, tile):
            ahead(rows_in, slice(start, start + tile))

    @pl.when(step > 0)
    def _():
        idx = step - 1

        @pl.when(stage == n_stages - 1)
        def _():
            gin[idx] = loss_ref[...]

        @pl.when(stage < n_stages - 1)
        def _():
            copy_of(idx).wait_recv()

        grad_in = gin[idx]
        gout_ref[...] = grad_in
        rows_in = acts_ref[...]
        flip_ref[...] = rows_in.T
        back = jnp.zeros(grad_in.shape, jnp.float32)
        for start in range(0, ff, tile):
            cols = slice(start, start + tile)
            d_pre = (mat_nt(grad_in, down_ref[cols, :]) * slope[:, cols]).astype(jnp.bfloat16)
            put_blocks(dpre_ref, start, d_pre)
            back = back + mat_nt(d_pre, up_ref[:, cols])
            ahead(rows_in, cols)

        @pl.when(stage > 0)
        def _():
            gsend[idx] = (grad_in.astype(jnp.float32) + back).astype(jnp.bfloat16)
            copy_of(idx).start()

    @pl.when((step == n_chunks) & (stage > 0))
    def _():
        for idx in range(n_chunks):
            copy_of(idx).wait_send()


def backward(n_stages, stage_in, master_up, master_down, loss_grad):
    rows, width = stage_in.shape
    ff = master_up.shape[1]
    n_chunks = rows // CHUNK

    def now(i):
        return jnp.minimum(i, n_chunks - 1)

    def late(i):
        return jnp.maximum(i - 1, 0)

    return pl.pallas_call(
        functools.partial(back_kernel, n_stages, n_chunks, TILE),
        grid=(n_chunks + 1,),
        out_shape=(
            jax.ShapeDtypeStruct((ff // LANES, rows, LANES), jnp.bfloat16),
            jax.ShapeDtypeStruct((ff // LANES, rows, LANES), jnp.bfloat16),
            jax.ShapeDtypeStruct((rows, width), jnp.bfloat16),
            jax.ShapeDtypeStruct((width, rows), jnp.bfloat16),
        ),
        in_specs=[
            pl.BlockSpec((CHUNK, width), lambda i: (now(i), 0)),
            pl.BlockSpec(memory_space=pltpu.VMEM),
            pl.BlockSpec(memory_space=pltpu.VMEM),
            pl.BlockSpec((CHUNK, width), lambda i: (late(i), 0)),
        ],
        out_specs=(
            pl.BlockSpec((ff // LANES, CHUNK, LANES), lambda i: (0, now(i), 0)),
            pl.BlockSpec((ff // LANES, CHUNK, LANES), lambda i: (0, late(i), 0)),
            pl.BlockSpec((CHUNK, width), lambda i: (late(i), 0)),
            pl.BlockSpec((width, CHUNK), lambda i: (0, now(i))),
        ),
        scratch_shapes=[
            pltpu.VMEM((width, ff), jnp.bfloat16),
            pltpu.VMEM((ff, width), jnp.bfloat16),
            pltpu.VMEM((n_chunks, CHUNK, width), jnp.bfloat16),
            pltpu.VMEM((n_chunks, CHUNK, width), jnp.bfloat16),
            pltpu.VMEM((CHUNK, ff), jnp.float32),
            pltpu.SemaphoreType.DMA((n_chunks,)),
            pltpu.SemaphoreType.DMA((n_chunks,)),
        ],
        compiler_params=pltpu.CompilerParams(collective_id=0, has_side_effects=True, dimension_semantics=('arbitrary',), vmem_limit_bytes=67043328),
        name='backward',
    )(stage_in, master_up, master_down, loss_grad)


def fwd_kernel(n_stages, n_chunks, tile, first_ref, up_ref, down_ref, out_ref, xin, xsend, send_sem, recv_sem):
    step = pl.program_id(0)
    rep = lax.axis_index('data')
    stage = lax.axis_index('stage')
    ff = up_ref.shape[1]
    enter(step, rep, stage, n_stages)

    def copy_of(idx):
        return pltpu.make_async_remote_copy(
            src_ref=xsend.at[idx],
            dst_ref=xin.at[idx],
            send_sem=send_sem.at[idx],
            recv_sem=recv_sem.at[idx],
            device_id=(rep, jnp.minimum(stage + 1, n_stages - 1)),
            device_id_type=MESH,
        )

    @pl.when(stage == 0)
    def _():
        xin[step] = first_ref[...]

    @pl.when(stage > 0)
    def _():
        copy_of(step).wait_recv()

    rows_in = xin[step]
    total = jnp.zeros(rows_in.shape, jnp.float32)
    for start in range(0, ff, tile):
        cols = slice(start, start + tile)
        hidden = gelu_tanh(mat_nn(rows_in, up_ref[:, cols])).astype(jnp.bfloat16)
        total = total + mat_nn(hidden, down_ref[cols, :])
    rows_out = (rows_in.astype(jnp.float32) + total).astype(jnp.bfloat16)
    out_ref[...] = rows_out

    @pl.when(stage < n_stages - 1)
    def _():
        xsend[step] = rows_out
        copy_of(step).start()

    @pl.when((step == n_chunks - 1) & (stage < n_stages - 1))
    def _():
        for idx in range(n_chunks):
            copy_of(idx).wait_send()


def forward(n_stages, first_in, up_bf, down_bf):
    rows, width = first_in.shape
    ff = up_bf.shape[1]
    n_chunks = rows // FWD_CHUNK
    row_spec = pl.BlockSpec((FWD_CHUNK, width), lambda i: (i, 0))
    return pl.pallas_call(
        functools.partial(fwd_kernel, n_stages, n_chunks, FWD_TILE),
        grid=(n_chunks,),
        out_shape=jax.ShapeDtypeStruct((rows, width), jnp.bfloat16),
        in_specs=[row_spec, pl.BlockSpec((width, ff), lambda i: (0, 0)), pl.BlockSpec((ff, width), lambda i: (0, 0))],
        out_specs=row_spec,
        scratch_shapes=[
            pltpu.VMEM((n_chunks, FWD_CHUNK, width), jnp.bfloat16),
            pltpu.VMEM((n_chunks, FWD_CHUNK, width), jnp.bfloat16),
            pltpu.SemaphoreType.DMA((n_chunks,)),
            pltpu.SemaphoreType.DMA((n_chunks,)),
        ],
        compiler_params=pltpu.CompilerParams(collective_id=1, has_side_effects=True, dimension_semantics=('arbitrary',), vmem_limit_bytes=60 * 2**20),
        name='forward',
    )(first_in, up_bf, down_bf)


def fold_squares(value):
    total = jnp.zeros((8, LANES), jnp.float32)
    for row in range(0, value.shape[0], 8):
        for col in range(0, value.shape[1], LANES):
            part = value[row : row + 8, col : col + LANES]
            total = total + part * part
    return total


def sum_kernel(n_chunks, skew, n_reps, flip_ref, dpre_hbm, hid_hbm, gown_ref, gup_hbm, gdown_hbm, out_up, out_down, sq_ref, acc_up, acc_down, dpre_buf, hid_buf, y_up, z_up, x_up, z_down, x_down, y_down, send_sem, recv_sem, last_sem, local_sem, load_sem, grad_sem, sq_part, sq_land, sq_send, sq_recv):
    rep = lax.axis_index('data')
    stage = lax.axis_index('stage')
    z_pos = rep // 2
    y_pos = rep % 2
    inner = (z_pos == 1) | (z_pos == 2)
    outer = jnp.logical_not(inner)
    partner = rep + 1 - 2 * y_pos
    low = z_pos < 2
    near = jnp.where(low, 1 - z_pos, 5 - z_pos) * 2 + y_pos
    across = jnp.where(inner, 3 - z_pos, z_pos) * 2 + y_pos
    own_half = jnp.where(low, 0, 1)
    n_blocks = n_chunks // 2
    up_rows = out_up.shape[0] // 4
    down_rows = out_down.shape[0] // (2 * n_chunks)

    def load_dpre(block):
        slot = lax.rem(block, 2)
        return pltpu.make_async_copy(dpre_hbm.at[block], dpre_buf.at[slot], load_sem.at[0, slot])

    def load_hid(block):
        slot = lax.rem(block, 2)
        return pltpu.make_async_copy(hid_hbm.at[block], hid_buf.at[slot], load_sem.at[1, slot])

    def load_gup(block):
        return pltpu.make_async_copy(gup_hbm.at[:, pl.ds(pl.multiple_of(block * LANES, LANES), LANES)], acc_up.at[block], grad_sem.at[0, block])

    def load_gdown(block):
        return pltpu.make_async_copy(gdown_hbm.at[pl.ds(pl.multiple_of(block * LANES, LANES), LANES)], acc_down.at[block], grad_sem.at[1, block])

    def build(block):
        slot = lax.rem(block, 2)
        load_dpre(block).wait()
        load_gup(block).wait()
        acc_up[block] = acc_up[block] + mat_nn(flip_ref[...], dpre_buf[slot])
        load_hid(block).wait()
        load_gdown(block).wait()
        acc_down[block] = acc_down[block] + mat_tn(hid_buf[slot], gown_ref[...])

        @pl.when(block + 2 < n_blocks)
        def _():
            load_dpre(block + 2).start()
            load_hid(block + 2).start()

    for block in range(2):
        load_dpre(block).start()
        load_gup(block).start()
        load_hid(block).start()
        load_gdown(block).start()

    def load_rest(block, carry):
        load_gup(block).start()
        load_gdown(block).start()
        return carry

    lax.fori_loop(2, n_blocks, load_rest, 0)
    sq_part[...] = jnp.zeros_like(sq_part)
    build(0)

    barrier = pltpu.get_barrier_semaphore()
    for hop in range(1, n_reps):
        pl.semaphore_signal(barrier, inc=1, device_id=(lax.rem(rep + hop, n_reps), stage), device_id_type=MESH)
    pl.semaphore_wait(barrier, n_reps - 1)

    def rows_at(idx, half):
        return pl.ds(pl.multiple_of((half * 2 + lax.rem(idx, 2)) * up_rows, up_rows), up_rows)

    def up_out(idx, half):
        return out_up.at[rows_at(idx, half), pl.ds(pl.multiple_of((idx // 2) * LANES, LANES), LANES)]

    def pair_at(idx):
        return pl.ds(pl.multiple_of(lax.rem(idx, 2) * (2 * down_rows), 2 * down_rows), 2 * down_rows)

    def down_at(idx, half):
        return pl.ds(pl.multiple_of(idx * (2 * down_rows) + half * down_rows, down_rows), down_rows)

    def half_at(half):
        return pl.ds(pl.multiple_of(half * down_rows, down_rows), down_rows)

    def remote(src, dst, send, recv, peer):
        return pltpu.make_async_remote_copy(src_ref=src, dst_ref=dst, send_sem=send_sem.at[send], recv_sem=recv, device_id=(peer, stage), device_id_type=MESH)

    def raw_up(idx):
        return remote(acc_up.at[idx // 2, rows_at(idx, 1 - y_pos)], y_up.at[idx], 0, recv_sem.at[0, idx], partner)

    def raw_down(idx):
        return remote(acc_down.at[idx // 2, pair_at(idx)], z_down.at[idx], 1, recv_sem.at[1, idx], near)

    def pair_up(idx):
        return remote(y_up.at[idx], z_up.at[idx], 2, recv_sem.at[2, idx], near)

    def part_down(idx):
        return remote(z_down.at[idx, half_at(1 - own_half)], x_down.at[idx], 3, recv_sem.at[3, idx], across)

    def part_up(idx):
        return remote(z_up.at[idx], x_up.at[idx], 4, recv_sem.at[4, idx], across)

    def rail_down(idx):
        return remote(x_down.at[idx], y_down.at[idx], 5, recv_sem.at[5, idx], partner)

    def done_up_near(idx):
        return remote(x_up.at[idx], up_out(idx, y_pos), 6, recv_sem.at[6, idx], near)

    def done_up_pair(idx):
        return remote(x_up.at[idx], up_out(idx, y_pos), 7, last_sem.at[0], partner)

    def done_down_near(idx):
        return remote(y_down.at[idx], out_down.at[down_at(idx, own_half)], 8, last_sem.at[1], near)

    def done_down_across(idx):
        return remote(y_down.at[idx], out_down.at[down_at(idx, own_half)], 9, recv_sem.at[7, idx], across)

    def pass_up(idx):
        return remote(up_out(idx, y_pos), up_out(idx, y_pos), 10, last_sem.at[0], partner)

    def pass_down(idx):
        rows = down_at(idx, 1 - own_half)
        return remote(out_down.at[rows], out_down.at[rows], 11, last_sem.at[1], near)

    def keep_up(idx):
        return pltpu.make_async_copy(x_up.at[idx], up_out(idx, y_pos), local_sem.at[0])

    def keep_down(idx):
        return pltpu.make_async_copy(y_down.at[idx], out_down.at[down_at(idx, own_half)], local_sem.at[1])

    def valid(idx):
        return (idx >= 0) & (idx < n_chunks)

    def tick(step, carry):
        @pl.when(valid(step))
        def _():
            raw_up(step).start()

            @pl.when(outer)
            def _():
                raw_down(step).start()

        first = step - skew

        @pl.when(valid(first))
        def _():
            raw_up(first).wait_recv()
            y_up[first] = y_up[first] + acc_up[first // 2, rows_at(first, y_pos), :]

            @pl.when(outer)
            def _():
                pair_up(first).start()

            @pl.when(inner)
            def _():
                raw_down(first).wait_recv()
                z_down[first] = z_down[first] + acc_down[first // 2, pair_at(first), :]
                part_down(first).start()

        second = step - 2 * skew

        @pl.when(valid(second) & inner)
        def _():
            pair_up(second).wait_recv()
            z_up[second] = z_up[second] + y_up[second]
            part_up(second).start()
            part_down(second).wait_recv()
            x_down[second] = x_down[second] + z_down[second, half_at(own_half), :]
            rail_down(second).start()

        third = step - 3 * skew

        @pl.when(valid(third) & inner)
        def _():
            part_up(third).wait_recv()
            total_up = x_up[third] + z_up[third]
            x_up[third] = total_up
            sq_part[0] = sq_part[0] + fold_squares(total_up / n_reps)
            done_up_near(third).start()
            done_up_pair(third).start()
            keep_up(third).start()
            rail_down(third).wait_recv()
            total_down = y_down[third] + x_down[third]
            y_down[third] = total_down
            sq_part[1] = sq_part[1] + fold_squares(total_down / n_reps)
            done_down_across(third).start()
            done_down_near(third).start()
            keep_down(third).start()

        fourth = step - 4 * skew

        @pl.when(valid(fourth) & outer)
        def _():
            done_up_near(fourth).wait_recv()
            pass_up(fourth).start()

        @pl.when(valid(fourth) & inner)
        def _():
            remote(y_down.at[fourth], out_down.at[down_at(fourth, 1 - own_half)], 9, recv_sem.at[7, fourth], across).wait_recv()
            pass_down(fourth).start()

        @pl.when((lax.rem(step, 2) == 1) & (step + 1 < n_chunks))
        def _():
            build((step + 1) // 2)

        return carry

    lax.fori_loop(0, n_chunks + 4 * skew, tick, 0)

    slot = jnp.where(low, 0, 2) + y_pos

    def square_copy(hop, source):
        return pltpu.make_async_remote_copy(src_ref=sq_land.at[source], dst_ref=sq_land.at[source], send_sem=sq_send.at[hop - 1], recv_sem=sq_recv.at[source], device_id=(lax.rem(rep + hop, n_reps), stage), device_id_type=MESH)

    @pl.when(inner)
    def _():
        sq_land[slot] = jnp.where(z_pos == 1, sq_part[0], 0.0) + jnp.where(y_pos == 0, sq_part[1], 0.0)
        for hop in range(1, n_reps):
            square_copy(hop, slot).start()

    up_half = pl.ds(0, out_up.shape[0] // 2)
    down_half = pl.ds(0, out_down.shape[0] // 2)

    def all_up(send, recv, peer):
        return remote(out_up.at[up_half], out_up.at[up_half], send, recv, peer)

    def all_down(send, recv, peer):
        return remote(out_down.at[down_half], out_down.at[down_half], send, recv, peer)

    all_up(0, last_sem.at[0], partner).wait_send()
    all_up(0, last_sem.at[0], partner).wait_recv()

    @pl.when(outer)
    def _():
        remote(out_down, out_down, 1, last_sem.at[1], near).wait_send()
        all_up(2, last_sem.at[0], near).wait_send()
        all_up(10, last_sem.at[0], partner).wait_send()
        remote(out_down, out_down, 1, last_sem.at[1], near).wait_recv()

    @pl.when(inner)
    def _():
        all_down(3, last_sem.at[1], across).wait_send()
        all_up(4, last_sem.at[0], across).wait_send()
        all_down(5, last_sem.at[1], partner).wait_send()
        all_up(6, last_sem.at[0], near).wait_send()
        all_up(7, last_sem.at[0], partner).wait_send()
        all_down(8, last_sem.at[1], near).wait_send()
        all_down(9, last_sem.at[1], across).wait_send()
        all_down(11, last_sem.at[1], near).wait_send()
        pltpu.make_async_copy(out_up.at[up_half], out_up.at[up_half], local_sem.at[0]).wait()
        pltpu.make_async_copy(out_down.at[down_half], out_down.at[down_half], local_sem.at[1]).wait()

    for source in range(4):
        @pl.when(rep != source + 2)
        def _():
            square_copy(1, source).wait_recv()

    @pl.when(inner)
    def _():
        for hop in range(1, n_reps):
            square_copy(hop, slot).wait_send()

    sq_ref[...] = sq_land[0] + sq_land[1] + sq_land[2] + sq_land[3]


def sum_grads(n_reps, flipped, dpre_own, hid_own, grad_own, grad_up, grad_down):
    width, ff = grad_up.shape
    rows = grad_own.shape[0]
    n_blocks = ff // LANES
    n_chunks = 2 * n_blocks
    up_land = pltpu.VMEM((n_chunks, width // 4, LANES), jnp.float32)
    down_land = pltpu.VMEM((n_chunks, LANES // 4, width), jnp.float32)
    vmem = pl.BlockSpec(memory_space=pltpu.VMEM)
    hbm = pl.BlockSpec(memory_space=pl.ANY)
    return pl.pallas_call(
        functools.partial(sum_kernel, n_chunks, SUM_SKEW, n_reps),
        out_shape=(jax.ShapeDtypeStruct(grad_up.shape, jnp.float32), jax.ShapeDtypeStruct(grad_down.shape, jnp.float32), jax.ShapeDtypeStruct((8, LANES), jnp.float32)),
        in_specs=[vmem, hbm, hbm, vmem, hbm, hbm],
        out_specs=(hbm, hbm, vmem),
        scratch_shapes=[
            pltpu.VMEM((n_blocks, width, LANES), jnp.float32),
            pltpu.VMEM((n_blocks, LANES, width), jnp.float32),
            pltpu.VMEM((2, rows, LANES), jnp.bfloat16),
            pltpu.VMEM((2, rows, LANES), jnp.bfloat16),
            up_land,
            up_land,
            up_land,
            pltpu.VMEM((n_chunks, LANES // 2, width), jnp.float32),
            down_land,
            down_land,
            pltpu.SemaphoreType.DMA((12,)),
            pltpu.SemaphoreType.DMA((8, n_chunks)),
            pltpu.SemaphoreType.DMA((2,)),
            pltpu.SemaphoreType.DMA((2,)),
            pltpu.SemaphoreType.DMA((2, 2)),
            pltpu.SemaphoreType.DMA((2, n_blocks)),
            pltpu.VMEM((2, 8, LANES), jnp.float32),
            pltpu.VMEM((4, 8, LANES), jnp.float32),
            pltpu.SemaphoreType.DMA((n_reps - 1,)),
            pltpu.SemaphoreType.DMA((4,)),
        ],
        compiler_params=pltpu.CompilerParams(collective_id=2, has_side_effects=True, vmem_limit_bytes=67043328),
        name='sum_grads',
    )(flipped, dpre_own, hid_own, grad_own, grad_up, grad_down)


def adam_kernel(n_reps, scale_ref, *refs):
    for start in range(2):
        master_ref, first_ref, second_ref, sum_ref = refs[4 * start : 4 * start + 4]
        new_master, new_first, new_second, new_bf = refs[8 + 4 * start : 12 + 4 * start]
        result, first_mom, second_mom = adamw_update(master_ref[...], first_ref[...], second_ref[...], sum_ref[...] / n_reps, scale_ref[0], scale_ref[1])
        new_master[...] = result
        new_first[...] = first_mom
        new_second[...] = second_mom
        new_bf[...] = result.astype(jnp.bfloat16)


def adam(n_reps, scales, up_arrays, down_arrays):
    in_specs, out_specs, shapes = [], [], []
    for arrays in (up_arrays, down_arrays):
        rows, cols = arrays[0].shape
        block = pl.BlockSpec((rows // ADAM_BLOCKS, cols), lambda i: (i, 0))
        full = jax.ShapeDtypeStruct((rows, cols), jnp.float32)
        in_specs += [block] * 4
        out_specs += [block] * 4
        shapes += [full, full, full, jax.ShapeDtypeStruct((rows, cols), jnp.bfloat16)]
    return pl.pallas_call(
        functools.partial(adam_kernel, n_reps),
        grid=(ADAM_BLOCKS,),
        out_shape=tuple(shapes),
        in_specs=[pl.BlockSpec(memory_space=pltpu.SMEM), *in_specs],
        out_specs=tuple(out_specs),
        compiler_params=pltpu.CompilerParams(dimension_semantics=('arbitrary',), vmem_limit_bytes=67043328),
        name='adam',
    )(scales, *up_arrays, *down_arrays)


def solution(mesh):
    n_stages = mesh.shape['stage']
    n_reps = mesh.shape['data']

    def local_step(master_up, master_down, mom1_up, mom1_down, mom2_up, mom2_down, grad_up, grad_down, stage_acts, loss_grad, next_batch, learn_rate, max_norm):
        stage_in = stage_acts[0]
        hid_own, dpre_own, grad_own, flipped = backward(n_stages, stage_in, master_up[0], master_down[0], loss_grad)
        sum_up, sum_down, squares = sum_grads(n_reps, flipped, dpre_own, hid_own, grad_own, grad_up[0, 0], grad_down[0, 0])
        grad_norm = jnp.sqrt(lax.psum(jnp.sum(squares), 'stage'))
        clip_scale = jnp.minimum(1.0, max_norm / (grad_norm + NORM_EPS))
        scales = jnp.stack([clip_scale, learn_rate])
        new_up, new_m1_up, new_m2_up, up_bf, new_down, new_m1_down, new_m2_down, down_bf = adam(
            n_reps, scales, (master_up[0], mom1_up[0], mom2_up[0], sum_up), (master_down[0], mom1_down[0], mom2_down[0], sum_down)
        )
        stage_out = forward(n_stages, next_batch[0], up_bf, down_bf)
        return (new_up[None], new_down[None], new_m1_up[None], new_m1_down[None], new_m2_up[None], new_m2_down[None], stage_out[None, None])

    w_spec = P('stage', None, None)
    g_spec = P('data', 'stage', None, None)
    in_specs = (w_spec, w_spec, w_spec, w_spec, w_spec, w_spec, g_spec, g_spec, P('stage', 'data', None), P('data', None), P(None, 'data', None), P(), P())
    out_specs = (w_spec, w_spec, w_spec, w_spec, w_spec, w_spec, P('stage', None, 'data', None))
    return jax.shard_map(local_step, mesh=mesh, in_specs=in_specs, out_specs=out_specs, check_vma=False)
```
